64 devices in a mesh: stage: 4 (over x, y), data: 16 (over z, core).
Axes of the slice: x: 2, y: 2, z: 8, core: 2. Of those that a mesh axis runs over, the one named last changes fastest.
The devices are a block of a 4x4x8 slice.
Arguments:
- w_master: float32 [128, 1536, 512], P('stage', 'data'), parts along dimension 0
- momentum: float32 [128, 1536, 512], P('stage', 'data'), parts along dimension 0
- grad: bfloat16 [128, 1536, 512], P('stage', 'data'), parts along dimension 0
Outputs:
- output 1: bfloat16 [128, 1536, 512], P('stage'), parts along dimension 0
- output 2: float32 [128, 1536, 512], P('stage', 'data'), parts along dimension 0
There are 4 independent parts. The reference program is written for one: setup_inputs(seed, part) draws one part's arguments, and reference() takes and returns one part's arrays. A program takes and returns all parts, laid end to end along the dimension named above; each array names one.
All inputs are finite; a program needn't handle non-finite values.
Results may differ from the reference program's by a relative error of at most 0.0073494.
Values are sent between devices in bfloat16 or wider.
A program may use at most 768 MiB of HBM per device.

```python
import math
import jax
import jax.numpy as jnp
from jax import lax

DATA_DEVS = 16
MATS_DEV = 2
D = 1536
FF_E = 512
NS_ITERS = 5

MOMENTUM = 0.95
LEARN_RATE = 0.02
WEIGHT_DECAY = 0.1
NORM_EPS = 1e-7
COEF_A = 3.4445
COEF_B = -4.7750
COEF_C = 2.0315
RMS_SCALE = 0.2 * math.sqrt(max(D, FF_E))


def setup_inputs(seed: int = 0, part: int = 0) -> dict:
    mat_count = MATS_DEV * DATA_DEVS
    key = jax.random.fold_in(jax.random.key(seed), part)
    keys = jax.random.split(key, 7)
    w_master = 0.02 * jax.random.normal(keys[0], (mat_count, D, FF_E), jnp.float32)
    left_fac = jax.random.normal(keys[1], (mat_count, D, 4), jnp.float32)
    right_fac = jax.random.normal(keys[2], (mat_count, 4, FF_E), jnp.float32)
    shared = 0.25 * jnp.einsum("mdr,mrf->mdf", left_fac, right_fac)
    row_scale = jax.random.uniform(keys[3], (mat_count, D, 1), jnp.float32, 0.5, 2.0)
    momentum = row_scale * (jax.random.normal(keys[4], (mat_count, D, FF_E), jnp.float32) + shared)
    grad_scale = jax.random.uniform(keys[5], (mat_count, D, 1), jnp.float32, 0.5, 2.0)
    grad = (grad_scale * jax.random.normal(keys[6], (mat_count, D, FF_E), jnp.float32)).astype(jnp.bfloat16)
    return {"w_master": w_master, "momentum": momentum, "grad": grad}


def newton_schulz(x_mat):
    for iteration in range(NS_ITERS):
        gram_mat = jnp.dot(x_mat, x_mat.T, preferred_element_type=jnp.float32).astype(jnp.bfloat16)
        square = jnp.dot(gram_mat, gram_mat, preferred_element_type=jnp.float32)
        poly_mat = (COEF_B * gram_mat.astype(jnp.float32) + COEF_C * square).astype(jnp.bfloat16)
        prod_mat = jnp.dot(poly_mat, x_mat, preferred_element_type=jnp.float32)
        x_mat = (COEF_A * x_mat.astype(jnp.float32) + prod_mat).astype(jnp.bfloat16)
    return x_mat


def orthogonalize(mom_one):
    frob_norm = jnp.sqrt(jnp.sum(mom_one * mom_one))
    x_mat = (mom_one.astype(jnp.bfloat16).astype(jnp.float32) / (frob_norm + NORM_EPS)).astype(jnp.bfloat16)
    if D > FF_E:
        x_mat = newton_schulz(x_mat.T).T
    else:
        x_mat = newton_schulz(x_mat)
    return x_mat.astype(jnp.float32) * RMS_SCALE


def reference(w_master, momentum, grad):
    mom_new = MOMENTUM * momentum + grad.astype(jnp.float32)

    def update_one(w_and_m):
        w_one, mom_one = w_and_m
        w_new = w_one - LEARN_RATE * (orthogonalize(mom_one) + WEIGHT_DECAY * w_one)
        return w_new.astype(jnp.bfloat16)

    params = lax.map(update_one, (w_master, mom_new))
    return params, mom_new
```

```python
import functools
import math
import jax
import jax.numpy as jnp
from jax import lax
from jax.experimental import pallas as pl
from jax.experimental.pallas import tpu as pltpu
from jax.sharding import PartitionSpec as P

NS_ITERS = 5
MOMENTUM = 0.95
LEARN_RATE = 0.02
WEIGHT_DECAY = 0.1
NORM_EPS = 1e-7
COEF_A = 3.4445
COEF_B = -4.7750
COEF_C = 2.0315
CORES = 2
QUADS = 4
MESH = pl.DeviceIdType.MESH
F32 = jnp.float32
BF16 = jnp.bfloat16


def hops(quad):
    return (4, 3) if quad % 2 == 0 else (3, 4)


def newton_schulz(x_ref, gram_ref, poly_ref, denom):
    blocks, rows, cols = x_ref.shape

    def scale(j, carry):
        x_ref[j] = (x_ref[j].astype(F32) / denom).astype(BF16)
        return carry

    lax.fori_loop(0, blocks, scale, 0)
    half = cols // 2
    step = blocks // 4

    def iteration(i, carry):
        x_all = x_ref[...].reshape(blocks * rows, cols)
        gram_ref[...] = lax.dot_general(
            x_all, x_all, (((0,), (0,)), ((), ())), preferred_element_type=F32
        ).astype(BF16)
        gram = gram_ref[...]
        for p in range(2):
            part = gram_ref[p * half:(p + 1) * half, :]
            square = jnp.dot(part, gram, preferred_element_type=F32)
            poly_ref[p * half:(p + 1) * half, :] = (COEF_B * part.astype(F32) + COEF_C * square).astype(BF16)
        poly = poly_ref[...]

        def rows_of(r, inner):
            x_part = x_ref[pl.ds(r * step, step)].reshape(step * rows, cols)
            prod = jnp.dot(x_part, poly, preferred_element_type=F32)
            x_ref[pl.ds(r * step, step)] = (COEF_A * x_part.astype(F32) + prod).astype(BF16).reshape(step, rows, cols)
            return inner

        for r in range(4):
            rows_of(r, 0)
        return carry

    lax.fori_loop(0, NS_ITERS, iteration, 0)


def step_kernel(group, w_hbm, mom_hbm, grad_hbm, out_hbm,
                mom_v, grad_v, w_v, mom_b, x_v, o_v, new_v, sq_out, sq_in, gram_v, poly_v,
                in_sem, w_sem, a_send, a_recv, q_send, q_recv, o_send, o_recv,
                ring_send, ring_recv, pair_send, pair_recv, own_sem):
    count, rows, cols = mom_hbm.shape
    chips = group // CORES
    quad_mats = group // QUADS
    rms = 0.2 * math.sqrt(max(rows * group, cols))
    me = lax.axis_index("data")
    chip, core = me // CORES, me % CORES
    up = lax.rem(chip + 1, chips) * CORES + core
    down = lax.rem(chip + chips - 1, chips) * CORES + core
    pair = chip * CORES + (1 - core)

    def peer(k):
        return lax.rem(me + k, group)

    def remote(src, dst, send_sem, recv_sem, to):
        return pltpu.make_async_remote_copy(src, dst, send_sem, recv_sem, device_id={"data": to}, device_id_type=MESH)

    for s in range(2):
        def load(k, carry):
            m = s * group + peer(k)
            pltpu.make_async_copy(mom_hbm.at[m], mom_v.at[m], in_sem.at[0, m]).start()
            pltpu.make_async_copy(grad_hbm.at[m], grad_v.at[m], in_sem.at[1, m]).start()
            return carry
        lax.fori_loop(0, group, load, 0)
    for s in range(2):
        pltpu.make_async_copy(w_hbm.at[pl.ds(s * group, group)], w_v.at[pl.ds(s * group, group)], w_sem.at[s]).start()

    barrier = pltpu.get_barrier_semaphore()

    def greet(k, carry):
        pl.semaphore_signal(barrier, inc=1, device_id={"data": peer(k)}, device_id_type=MESH)
        return carry
    lax.fori_loop(1, group, greet, 0)
    pl.semaphore_wait(barrier, group - 1)

    for s in range(2):
        def send(k):
            to = peer(k)
            m = s * group + to
            remote(mom_b.at[m], x_v.at[s, me], a_send.at[s], a_recv.at[s], to).start()
            remote(sq_out.at[m], sq_in.at[s, me], q_send.at[s], q_recv.at[s], to).start()

        def momentum(k, carry):
            m = s * group + peer(k)
            pltpu.make_async_copy(mom_hbm.at[m], mom_v.at[m], in_sem.at[0, m]).wait()
            pltpu.make_async_copy(grad_hbm.at[m], grad_v.at[m], in_sem.at[1, m]).wait()
            new = MOMENTUM * mom_v[m] + grad_v[m].astype(F32)
            sq = (new * new).reshape(rows // 8, 8, cols // 128, 128)
            sq_out[m] = jnp.sum(jnp.sum(sq, axis=0), axis=1)
            mom_b[m] = new.astype(BF16)

            @pl.when(k > 1)
            def _():
                send(k - 1)
            return carry
        lax.fori_loop(0, group, momentum, 0)
        x_v[s, me] = mom_b[s * group + me]
        sq_in[s, me] = sq_out[s * group + me]
        send(group - 1)

    def owned(s, carry):
        others = pl.ds(0, group - 1)
        pltpu.make_async_copy(x_v.at[s, others], x_v.at[s, others], a_recv.at[s]).wait()
        pltpu.make_async_copy(sq_in.at[s, others], sq_in.at[s, others], q_recv.at[s]).wait()
        total = jnp.sum(jnp.sum(sq_in[s], axis=0), axis=0, keepdims=True)
        denom = jnp.sqrt(jnp.sum(total, axis=1, keepdims=True)) + NORM_EPS
        newton_schulz(x_v.at[s], gram_v, poly_v, denom)
        o_v[s * group + me] = x_v[s, me]

        def back(k, inner):
            to = peer(k)
            remote(x_v.at[s, to], o_v.at[s * group + me], o_send.at[s], o_recv.at[s], to).start()
            return inner
        lax.fori_loop(1, group, back, 0)
        return carry
    lax.fori_loop(0, 2, owned, 0)

    def block(ref, s, q, src):
        return ref.at[pl.ds(s * group + q * quad_mats, quad_mats), pl.ds(pl.multiple_of(src * rows, 32), rows), :]

    def update(s):
        others = pl.ds(0, group - 1)
        pltpu.make_async_copy(o_v.at[others], o_v.at[others], o_recv.at[s]).wait()
        pltpu.make_async_copy(w_hbm.at[pl.ds(s * group, group)], w_v.at[pl.ds(s * group, group)], w_sem.at[s]).wait()

        def one(m, carry):
            w_old = w_v[m]
            new_v[m] = (w_old - LEARN_RATE * (o_v[m].astype(F32) * rms + WEIGHT_DECAY * w_old)).astype(BF16)
            return carry
        lax.fori_loop(s * group, (s + 1) * group, one, 0)
        for q in range(QUADS):
            src = new_v.at[pl.ds(s * group + q * quad_mats, quad_mats)]
            dst = block(out_hbm, s, q, me)
            remote(src, dst, ring_send.at[0], ring_recv.at[0, s, q, 0], up).start()
            remote(src, dst, ring_send.at[1], ring_recv.at[1, s, q, 0], down).start()
            remote(src, dst, pair_send.at[0], pair_recv.at[0], pair).start()
            pltpu.make_async_copy(src, dst, own_sem.at[s]).start()

    def relay(s, h):
        for q in range(QUADS):
            for way in range(2):
                if h > hops(q)[way]:
                    continue
                src = lax.rem(chip + (chips - h if way == 0 else h), chips) * CORES + core
                blk = block(out_hbm, s, q, src)
                remote(blk, blk, ring_send.at[way], ring_recv.at[way, s, q, h - 1], (up, down)[way]).wait_recv()
                if h < hops(q)[way]:
                    remote(blk, blk, ring_send.at[way], ring_recv.at[way, s, q, h], (up, down)[way]).start()
                remote(blk, blk, pair_send.at[0], pair_recv.at[0], pair).start()

    update(0)
    relay(0, 1)
    update(1)
    relay(0, 2)
    relay(1, 1)
    relay(0, 3)
    relay(1, 2)
    relay(0, 4)
    relay(1, 3)
    relay(1, 4)

    others = pl.ds(0, group - 1)
    for s in range(2):
        pltpu.make_async_copy(x_v.at[s, others], x_v.at[s, others], a_send.at[s]).wait()
        pltpu.make_async_copy(sq_in.at[s, others], sq_in.at[s, others], q_send.at[s]).wait()
        pltpu.make_async_copy(o_v.at[others], o_v.at[others], o_send.at[s]).wait()
        own = new_v.at[pl.ds(s * group, group)]
        pltpu.make_async_copy(own, own, own_sem.at[s]).wait()
    for way in range(2):
        sent = sum(hops(q)[way] for q in range(QUADS)) * quad_mats * 2
        full = out_hbm.at[pl.ds(0, sent // group)]
        pltpu.make_async_copy(full, full, ring_send.at[way]).wait()
    full = out_hbm.at[pl.ds(0, count // 2)]
    pltpu.make_async_copy(full, full, pair_send.at[0]).wait()
    pltpu.make_async_copy(full, full, pair_recv.at[0]).wait()


def run_step(group, w_rows, mom_rows, grad_rows):
    count, rows, cols = mom_rows.shape
    any_spec = pl.BlockSpec(memory_space=pltpu.HBM)
    dma = pltpu.SemaphoreType.DMA
    return pl.pallas_call(
        functools.partial(step_kernel, group),
        out_shape=jax.ShapeDtypeStruct((count, rows * group, cols), BF16),
        in_specs=[any_spec] * 3,
        out_specs=any_spec,
        scratch_shapes=[
            pltpu.VMEM((count, rows, cols), F32),
            pltpu.VMEM((count, rows, cols), BF16),
            pltpu.VMEM((count, rows, cols), F32),
            pltpu.VMEM((count, rows, cols), BF16),
            pltpu.VMEM((2, group, rows, cols), BF16),
            pltpu.VMEM((count, rows, cols), BF16),
            pltpu.VMEM((count, rows, cols), BF16),
            pltpu.VMEM((count, 8, 128), F32),
            pltpu.VMEM((2, group, 8, 128), F32),
            pltpu.VMEM((cols, cols), BF16),
            pltpu.VMEM((cols, cols), BF16),
            dma((2, count)), dma((2,)),
            dma((2,)), dma((2,)), dma((2,)), dma((2,)), dma((2,)), dma((2,)),
            dma((2,)), dma((2, 2, QUADS, 4)), dma((1,)), dma((1,)), dma((2,)),
        ],
        compiler_params=pltpu.CompilerParams(collective_id=0, has_side_effects=True, vmem_limit_bytes=60 * 1024 * 1024),
        name="muon_step",
    )(w_rows, mom_rows, grad_rows)


def solution(mesh):
    group = mesh.shape["data"]
    row_spec = P("stage", "data", None)
    full_spec = P("stage", None, None)

    def local_step(w_rows, mom_rows, grad_rows):
        mom_new = MOMENTUM * mom_rows + grad_rows.astype(F32)
        params = run_step(group, w_rows, mom_rows, grad_rows)
        return params, mom_new

    return jax.shard_map(local_step, mesh=mesh, in_specs=(row_spec, row_spec, row_spec), out_specs=(full_spec, row_spec), check_vma=False)
```

```python
import functools
import math
import jax
import jax.numpy as jnp
from jax import lax
from jax.experimental import pallas as pl
from jax.experimental.pallas import tpu as pltpu
from jax.sharding import PartitionSpec as P

NS_ITERS = 5
MOMENTUM = 0.95
LEARN_RATE = 0.02
WEIGHT_DECAY = 0.1
NORM_EPS = 1e-7
COEF_A = 3.4445
COEF_B = -4.7750
COEF_C = 2.0315
CORES = 2
QUADS = 4
MESH = pl.DeviceIdType.MESH
F32 = jnp.float32
BF16 = jnp.bfloat16


RING_HOPS = 3
SLOTS = 12
LAG = 6


def newton_schulz(x_ref, gram_ref, poly_ref, denom):
    blocks, rows, cols = x_ref.shape

    def scale(j, carry):
        x_ref[j] = (x_ref[j].astype(F32) / denom).astype(BF16)
        return carry

    lax.fori_loop(0, blocks, scale, 0)
    half = cols // 2
    step = blocks // 4

    def iteration(i, carry):
        x_all = x_ref[...].reshape(blocks * rows, cols)
        gram_ref[...] = lax.dot_general(
            x_all, x_all, (((0,), (0,)), ((), ())), preferred_element_type=F32
        ).astype(BF16)
        gram = gram_ref[...]
        for p in range(2):
            part = gram_ref[p * half:(p + 1) * half, :]
            square = jnp.dot(part, gram, preferred_element_type=F32)
            poly_ref[p * half:(p + 1) * half, :] = (COEF_B * part.astype(F32) + COEF_C * square).astype(BF16)
        poly = poly_ref[...]

        def rows_of(r, inner):
            x_part = x_ref[pl.ds(r * step, step)].reshape(step * rows, cols)
            prod = jnp.dot(x_part, poly, preferred_element_type=F32)
            x_ref[pl.ds(r * step, step)] = (COEF_A * x_part.astype(F32) + prod).astype(BF16).reshape(step, rows, cols)
            return inner

        for r in range(4):
            rows_of(r, 0)
        return carry

    lax.fori_loop(0, NS_ITERS, iteration, 0)


def step_kernel(group, w_hbm, mom_hbm, grad_hbm, out_hbm, far_up, far_down,
                mom_v, grad_v, w_v, mom_b, x_v, o_v, new_v, sq_out, sq_in, gram_v, poly_v,
                in_sem, w_sem, a_send, a_recv, q_send, q_recv, o_send, o_recv,
                ring_send, ring_recv, pair_send, pair_recv, own_sem):
    count, rows, cols = mom_hbm.shape
    chips = group // CORES
    quad_mats = group // QUADS
    rms = 0.2 * math.sqrt(max(rows * group, cols))
    me = lax.axis_index("data")
    chip, core = me // CORES, me % CORES
    up = lax.rem(chip + 1, chips) * CORES + core
    down = lax.rem(chip + chips - 1, chips) * CORES + core
    pair = chip * CORES + (1 - core)

    def peer(k):
        return lax.rem(me + k, group)

    def remote(src, dst, send_sem, recv_sem, to):
        return pltpu.make_async_remote_copy(src, dst, send_sem, recv_sem, device_id={"data": to}, device_id_type=MESH)

    for s in range(2):
        def load(k, carry):
            m = s * group + peer(k)
            pltpu.make_async_copy(mom_hbm.at[m], mom_v.at[m], in_sem.at[0, m]).start()
            pltpu.make_async_copy(grad_hbm.at[m], grad_v.at[m], in_sem.at[1, m]).start()
            return carry
        lax.fori_loop(0, group, load, 0)
    for s in range(2):
        pltpu.make_async_copy(w_hbm.at[pl.ds(s * group, group)], w_v.at[pl.ds(s * group, group)], w_sem.at[s]).start()

    barrier = pltpu.get_barrier_semaphore()

    def greet(k, carry):
        pl.semaphore_signal(barrier, inc=1, device_id={"data": peer(k)}, device_id_type=MESH)
        return carry
    lax.fori_loop(1, group, greet, 0)
    pl.semaphore_wait(barrier, group - 1)

    for s in range(2):
        def send(k):
            to = peer(k)
            m = s * group + to
            remote(mom_b.at[m], x_v.at[s, me], a_send.at[s], a_recv.at[s], to).start()
            remote(sq_out.at[m], sq_in.at[s, me], q_send.at[s], q_recv.at[s], to).start()

        def momentum(k, carry):
            m = s * group + peer(k)
            pltpu.make_async_copy(mom_hbm.at[m], mom_v.at[m], in_sem.at[0, m]).wait()
            pltpu.make_async_copy(grad_hbm.at[m], grad_v.at[m], in_sem.at[1, m]).wait()
            new = MOMENTUM * mom_v[m] + grad_v[m].astype(F32)
            sq = (new * new).reshape(rows // 8, 8, cols // 128, 128)
            sq_out[m] = jnp.sum(jnp.sum(sq, axis=0), axis=1)
            mom_b[m] = new.astype(BF16)

            @pl.when(k > 1)
            def _():
                send(k - 1)
            return carry
        lax.fori_loop(0, group, momentum, 0)
        x_v[s, me] = mom_b[s * group + me]
        sq_in[s, me] = sq_out[s * group + me]
        send(group - 1)

    def owned(s, carry):
        others = pl.ds(0, group - 1)
        pltpu.make_async_copy(x_v.at[s, others], x_v.at[s, others], a_recv.at[s]).wait()
        pltpu.make_async_copy(sq_in.at[s, others], sq_in.at[s, others], q_recv.at[s]).wait()
        total = jnp.sum(jnp.sum(sq_in[s], axis=0), axis=0, keepdims=True)
        denom = jnp.sqrt(jnp.sum(total, axis=1, keepdims=True)) + NORM_EPS
        newton_schulz(x_v.at[s], gram_v, poly_v, denom)
        o_v[s * group + me] = x_v[s, me]

        def back(k, inner):
            to = peer(k)
            remote(x_v.at[s, to], o_v.at[s * group + me], o_send.at[s], o_recv.at[s], to).start()
            return inner
        lax.fori_loop(1, group, back, 0)
        return carry
    lax.fori_loop(0, 2, owned, 0)

    def block(ref, s, q, src):
        return ref.at[pl.ds(s * group + q * quad_mats, quad_mats), pl.ds(pl.multiple_of(src * rows, 32), rows), :]

    def update(s):
        others = pl.ds(0, group - 1)
        pltpu.make_async_copy(o_v.at[others], o_v.at[others], o_recv.at[s]).wait()
        pltpu.make_async_copy(w_hbm.at[pl.ds(s * group, group)], w_v.at[pl.ds(s * group, group)], w_sem.at[s]).wait()

        def one(m, carry):
            w_old = w_v[m]
            new_v[m] = (w_old - LEARN_RATE * (o_v[m].astype(F32) * rms + WEIGHT_DECAY * w_old)).astype(BF16)
            return carry
        lax.fori_loop(s * group, (s + 1) * group, one, 0)
        for q in range(QUADS):
            src = new_v.at[pl.ds(s * group + q * quad_mats, quad_mats)]
            dst = block(out_hbm, s, q, me)
            remote(src, dst, ring_send.at[0], ring_recv.at[0, s, q, 0], up).start()
            remote(src, dst, ring_send.at[1], ring_recv.at[1, s, q, 0], down).start()
            remote(src, dst, pair_send.at[0], pair_recv.at[0], pair).start()
            pltpu.make_async_copy(src, dst, own_sem.at[s]).start()

    def landing(s, q, way, h, src):
        if h == RING_HOPS and q % 2 == way:
            return (far_up, far_down)[way].at[pl.ds((s * (QUADS // 2) + q // 2) * quad_mats, quad_mats)]
        return block(out_hbm, s, q, src)

    def relay(s, h):
        for q in range(QUADS):
            for way in range(2):
                src = lax.rem(chip + (chips - h if way == 0 else h), chips) * CORES + core
                got = landing(s, q, way, h, src)
                remote(got, got, ring_send.at[way], ring_recv.at[way, s, q, h - 1], (up, down)[way]).wait_recv()
                if h < RING_HOPS:
                    remote(got, landing(s, q, way, h + 1, src), ring_send.at[way], ring_recv.at[way, s, q, h], (up, down)[way]).start()
                remote(got, block(out_hbm, s, q, src), pair_send.at[0], pair_recv.at[0], pair).start()

    update(0)
    relay(0, 1)
    update(1)
    relay(0, 2)
    relay(1, 1)
    relay(0, 3)
    relay(1, 2)
    relay(1, 3)

    others = pl.ds(0, group - 1)
    for s in range(2):
        pltpu.make_async_copy(x_v.at[s, others], x_v.at[s, others], a_send.at[s]).wait()
        pltpu.make_async_copy(sq_in.at[s, others], sq_in.at[s, others], q_send.at[s]).wait()
        pltpu.make_async_copy(o_v.at[others], o_v.at[others], o_send.at[s]).wait()
        own = new_v.at[pl.ds(s * group, group)]
        pltpu.make_async_copy(own, own, own_sem.at[s]).wait()
    for way in range(2):
        full = out_hbm.at[pl.ds(0, RING_HOPS * count // group)]
        pltpu.make_async_copy(full, full, ring_send.at[way]).wait()
    full = out_hbm.at[pl.ds(0, (2 * RING_HOPS + 1) * count // group)]
    pltpu.make_async_copy(full, full, pair_send.at[0]).wait()
    pltpu.make_async_copy(full, full, pair_recv.at[0]).wait()


def assemble_kernel(group, gath, far_up, far_down, mom_hbm, grad_hbm, out_hbm, mom_out,
                    buf, mom_v, grad_v, in_sem, out_sem, mom_in, mom_done):
    count, rows, cols = mom_hbm.shape
    chips = group // CORES
    quads = 2 * QUADS
    quad_mats = count // quads
    me = lax.axis_index("data")
    chip, core = me // CORES, me % CORES
    per_chip = CORES * quads
    total = (2 * RING_HOPS + 1) * per_chip
    every = total // quads

    def where(i):
        j, c, g = i // per_chip, (i // quads) % CORES, i % quads
        src = lax.rem(chip + j + chips - RING_HOPS, chips) * CORES + c
        return j, c, g, src

    def block(ref, g, src):
        return ref.at[pl.ds(g * quad_mats, quad_mats), pl.ds(pl.multiple_of(src * rows, 32), rows), :]

    def load(i):
        j, c, g, src = where(i)
        slot = i % SLOTS
        up_far = (j == 0) & (c == core) & (g % 2 == 0)
        down_far = (j == 2 * RING_HOPS) & (c == core) & (g % 2 == 1)
        far = pl.ds((g // 2) * quad_mats, quad_mats)

        @pl.when(up_far)
        def _():
            pltpu.make_async_copy(far_up.at[far], buf.at[slot], in_sem.at[slot]).start()

        @pl.when(down_far)
        def _():
            pltpu.make_async_copy(far_down.at[far], buf.at[slot], in_sem.at[slot]).start()

        @pl.when(jnp.logical_not(up_far | down_far))
        def _():
            pltpu.make_async_copy(block(gath, g, src), buf.at[slot], in_sem.at[slot]).start()

    def store(i):
        _, _, g, src = where(i)
        slot = i % SLOTS
        return pltpu.make_async_copy(buf.at[slot], block(out_hbm, g, src), out_sem.at[slot])

    def step(i, carry):
        slot = i % SLOTS

        @pl.when((i >= SLOTS) & (i < total))
        def _():
            store(i - SLOTS).wait()

        @pl.when(i < total)
        def _():
            load(i)

        @pl.when(i >= LAG)
        def _():
            late = (i - LAG) % SLOTS
            pltpu.make_async_copy(buf.at[late], buf.at[late], in_sem.at[late]).wait()
            store(i - LAG).start()

        t = i // every
        mats = pl.ds(t * quad_mats, quad_mats)

        @pl.when((i % every == 0) & (i < total))
        def _():
            pltpu.make_async_copy(mom_hbm.at[mats], mom_v.at[mats], mom_in.at[0, t]).start()
            pltpu.make_async_copy(grad_hbm.at[mats], grad_v.at[mats], mom_in.at[1, t]).start()

        @pl.when((i % every == every - 1) & (i < total))
        def _():
            pltpu.make_async_copy(mom_hbm.at[mats], mom_v.at[mats], mom_in.at[0, t]).wait()
            pltpu.make_async_copy(grad_hbm.at[mats], grad_v.at[mats], mom_in.at[1, t]).wait()

            def one(m, inner):
                mom_v[m] = MOMENTUM * mom_v[m] + grad_v[m].astype(F32)
                return inner
            lax.fori_loop(t * quad_mats, (t + 1) * quad_mats, one, 0)
            pltpu.make_async_copy(mom_v.at[mats], mom_out.at[mats], mom_done.at[t]).start()
        return carry

    lax.fori_loop(0, total + LAG, step, 0)

    def drain(i, carry):
        store(i).wait()
        return carry
    lax.fori_loop(total - SLOTS, total, drain, 0)
    for t in range(quads):
        mats = pl.ds(t * quad_mats, quad_mats)
        pltpu.make_async_copy(mom_v.at[mats], mom_out.at[mats], mom_done.at[t]).wait()


def place_kernel(group, other_core, prev, even, odd, out_hbm, buf, in_sem, out_sem):
    count = prev.shape[0]
    _, rows, _ = even.shape
    chips = group // CORES
    quads = 2 * QUADS
    quad_mats = count // quads
    me = lax.axis_index("data")
    chip, core = me // CORES, me % CORES
    src = lax.rem(chip + chips // 2, chips) * CORES + (1 - core if other_core else core)

    def load(g):
        ref = (even, odd)[g % 2]
        return pltpu.make_async_copy(ref.at[pl.ds((g // 2) * quad_mats, quad_mats)], buf.at[g], in_sem.at[g])

    def store(g):
        rows_of = pl.ds(pl.multiple_of(src * rows, 32), rows)
        return pltpu.make_async_copy(buf.at[g], out_hbm.at[pl.ds(g * quad_mats, quad_mats), rows_of, :], out_sem.at[g])

    for g in range(quads):
        load(g).start()
    for g in range(quads):
        load(g).wait()
        store(g).start()
    for g in range(quads):
        store(g).wait()


def assemble(group, gath, far_up, far_down, mom_rows, grad_rows):
    count, rows, cols = mom_rows.shape
    quads = 2 * QUADS
    any_spec = pl.BlockSpec(memory_space=pltpu.HBM)
    dma = pltpu.SemaphoreType.DMA
    return pl.pallas_call(
        functools.partial(assemble_kernel, group),
        out_shape=(jax.ShapeDtypeStruct(gath.shape, BF16), jax.ShapeDtypeStruct((count, rows, cols), F32)),
        in_specs=[any_spec] * 5,
        out_specs=(any_spec, any_spec),
        scratch_shapes=[
            pltpu.VMEM((SLOTS, count // quads, rows, cols), BF16),
            pltpu.VMEM((count, rows, cols), F32),
            pltpu.VMEM((count, rows, cols), BF16),
            dma((SLOTS,)), dma((SLOTS,)), dma((2, quads)), dma((quads,)),
        ],
        compiler_params=pltpu.CompilerParams(vmem_limit_bytes=60 * 1024 * 1024),
        cost_estimate=pl.CostEstimate(flops=200_000_000, bytes_accessed=4 * gath.size, transcendentals=0),
        name="assemble",
    )(gath, far_up, far_down, mom_rows, grad_rows)


def place(group, other_core, prev, even, odd):
    count = prev.shape[0]
    quads = 2 * QUADS
    any_spec = pl.BlockSpec(memory_space=pltpu.HBM)
    dma = pltpu.SemaphoreType.DMA
    return pl.pallas_call(
        functools.partial(place_kernel, group, other_core),
        out_shape=jax.ShapeDtypeStruct(prev.shape, BF16),
        in_specs=[any_spec] * 3,
        out_specs=any_spec,
        input_output_aliases={0: 0},
        scratch_shapes=[pltpu.VMEM((quads, count // quads) + even.shape[1:], BF16), dma((quads,)), dma((quads,))],
        cost_estimate=pl.CostEstimate(flops=20_000_000, bytes_accessed=8 * even.size, transcendentals=0),
        name="place_other" if other_core else "place_own",
    )(prev, even, odd)


def run_step(group, w_rows, mom_rows, grad_rows):
    count, rows, cols = mom_rows.shape
    any_spec = pl.BlockSpec(memory_space=pltpu.HBM)
    dma = pltpu.SemaphoreType.DMA
    return pl.pallas_call(
        functools.partial(step_kernel, group),
        out_shape=(
            jax.ShapeDtypeStruct((count, rows * group, cols), BF16),
            jax.ShapeDtypeStruct((count // 2, rows, cols), BF16),
            jax.ShapeDtypeStruct((count // 2, rows, cols), BF16),
        ),
        in_specs=[any_spec] * 3,
        out_specs=(any_spec,) * 3,
        scratch_shapes=[
            pltpu.VMEM((count, rows, cols), F32),
            pltpu.VMEM((count, rows, cols), BF16),
            pltpu.VMEM((count, rows, cols), F32),
            pltpu.VMEM((count, rows, cols), BF16),
            pltpu.VMEM((2, group, rows, cols), BF16),
            pltpu.VMEM((count, rows, cols), BF16),
            pltpu.VMEM((count, rows, cols), BF16),
            pltpu.VMEM((count, 8, 128), F32),
            pltpu.VMEM((2, group, 8, 128), F32),
            pltpu.VMEM((cols, cols), BF16),
            pltpu.VMEM((cols, cols), BF16),
            dma((2, count)), dma((2,)),
            dma((2,)), dma((2,)), dma((2,)), dma((2,)), dma((2,)), dma((2,)),
            dma((2,)), dma((2, 2, QUADS, RING_HOPS)), dma((1,)), dma((1,)), dma((2,)),
        ],
        compiler_params=pltpu.CompilerParams(collective_id=0, has_side_effects=True, vmem_limit_bytes=60 * 1024 * 1024),
        name="muon_step",
    )(w_rows, mom_rows, grad_rows)


def solution(mesh):
    group = mesh.shape["data"]
    row_spec = P("stage", "data", None)
    full_spec = P("stage", None, None)

    def local_step(w_rows, mom_rows, grad_rows):
        gath, far_up, far_down = run_step(group, w_rows, mom_rows, grad_rows)
        last_up = lax.ppermute(far_up, "data", [(d, (d + CORES) % group) for d in range(group)])
        last_down = lax.ppermute(far_down, "data", [(d, (d - CORES) % group) for d in range(group)])
        params, mom_new = assemble(group, gath, far_up, far_down, mom_rows, grad_rows)
        last_up, last_down, params = lax.optimization_barrier((last_up, last_down, params))
        pairs = [(d, d ^ 1) for d in range(group)]
        pair_up = lax.ppermute(last_up, "data", pairs)
        pair_down = lax.ppermute(last_down, "data", pairs)
        params = place(group, False, params, last_up, last_down)
        params = place(group, True, params, pair_up, pair_down)
        return params, mom_new

    return jax.shard_map(local_step, mesh=mesh, in_specs=(row_spec, row_spec, row_spec), out_specs=(full_spec, row_spec), check_vma=False)
```

```python
import functools
import math
import jax
import jax.numpy as jnp
from jax import lax
from jax.experimental import pallas as pl
from jax.experimental.pallas import tpu as pltpu
from jax.sharding import PartitionSpec as P

NS_ITERS = 5
MOMENTUM = 0.95
LEARN_RATE = 0.02
WEIGHT_DECAY = 0.1
NORM_EPS = 1e-7
COEF_A = 3.4445
COEF_B = -4.7750
COEF_C = 2.0315
CORES = 2
QUADS = 4
MESH = pl.DeviceIdType.MESH
F32 = jnp.float32
BF16 = jnp.bfloat16


RING_HOPS = 3
HELD = (QUADS - 1, QUADS - 2)
LAID_FIRST = 100
SLOTS = 12
LAG = 6


def newton_schulz(x_ref, gram_ref, poly_ref):
    blocks, rows, cols = x_ref.shape
    half = cols // 2
    step = blocks // 4

    def iteration(i, carry):
        x_all = x_ref[...].reshape(blocks * rows, cols)
        gram_ref[...] = lax.dot_general(
            x_all, x_all, (((0,), (0,)), ((), ())), preferred_element_type=F32
        ).astype(BF16)
        gram = gram_ref[...]
        for p in range(2):
            part = gram_ref[p * half:(p + 1) * half, :]
            square = jnp.dot(part, gram, preferred_element_type=F32)
            poly_ref[p * half:(p + 1) * half, :] = (COEF_B * part.astype(F32) + COEF_C * square).astype(BF16)
        poly = poly_ref[...]

        def rows_of(r, inner):
            x_part = x_ref[pl.ds(r * step, step)].reshape(step * rows, cols)
            prod = jnp.dot(x_part, poly, preferred_element_type=F32)
            x_ref[pl.ds(r * step, step)] = (COEF_A * x_part.astype(F32) + prod).astype(BF16).reshape(step, rows, cols)
            return inner

        for r in range(4):
            rows_of(r, 0)
        return carry

    lax.fori_loop(0, NS_ITERS, iteration, 0)


def step_kernel(group, w_hbm, mom_hbm, grad_hbm, out_hbm, far_up, far_down, near_up, near_down,
                mom_v, grad_v, w_v, mom_b, x_v, x_hold, o_v, o_hold, new_v, sq_out, sq_pair, sq_sum, sq_in, gram_v, poly_v,
                in_sem, w_sem, a_send, a_recv, ap_send, ap_recv, q_send, q_recv, qp_send, qp_recv,
                o_send, o_recv, op_send, op_recv, ring_send, ring_recv, pair_send, pair_recv, own_sem):
    _, rows, cols = mom_hbm.shape
    chips = group // CORES
    quad_mats = group // QUADS
    rms = 0.2 * math.sqrt(max(rows * group, cols))
    me = lax.axis_index("data")
    chip, core = me // CORES, me % CORES
    up = lax.rem(chip + 1, chips) * CORES + core
    down = lax.rem(chip + chips - 1, chips) * CORES + core
    pair = chip * CORES + (1 - core)

    def chip_at(i):
        return lax.rem(chip + chips // 2 + (i + 1) // 2 * (1 - 2 * (i % 2)), chips)

    def remote(src, dst, send_sem, recv_sem, to):
        return pltpu.make_async_remote_copy(src, dst, send_sem, recv_sem, device_id={"data": to}, device_id_type=MESH)

    barrier = pltpu.get_barrier_semaphore()

    def greet(i, carry):
        pl.semaphore_signal(barrier, inc=1, device_id={"data": chip_at(i) * CORES + core}, device_id_type=MESH)
        return carry

    lax.fori_loop(0, chips - 1, greet, 0)
    pl.semaphore_signal(barrier, inc=1, device_id={"data": pair}, device_id_type=MESH)

    def load_set(s):
        def load(i, carry):
            for cc in range(CORES):
                m = s * group + chip_at(i) * CORES + cc
                pltpu.make_async_copy(mom_hbm.at[m], mom_v.at[m], in_sem.at[0, m]).start()
                pltpu.make_async_copy(grad_hbm.at[m], grad_v.at[m], in_sem.at[1, m]).start()
            return carry

        lax.fori_loop(0, chips, load, 0)

    load_set(0)
    pl.semaphore_wait(barrier, chips)

    def send(s, i):
        to = chip_at(i)
        src = mom_b.at[pl.ds(s * group + to * CORES, CORES)]
        remote(src, x_hold.at[s, chip], a_send.at[s], a_recv.at[s, chip], to * CORES + core).start()

    def send_pair(s):
        remote(mom_b.at[s * group + pair], x_v.at[s, me], ap_send.at[s], ap_recv.at[s], pair).start()
        x_hold[s, chip, core] = mom_b[s * group + me]

    for s in range(2):
        def momentum(i, carry):
            to = chip_at(i)
            for cc in range(CORES):
                m = s * group + to * CORES + cc
                pltpu.make_async_copy(mom_hbm.at[m], mom_v.at[m], in_sem.at[0, m]).wait()
                pltpu.make_async_copy(grad_hbm.at[m], grad_v.at[m], in_sem.at[1, m]).wait()
                new = MOMENTUM * mom_v[m] + grad_v[m].astype(F32)
                sq = (new * new).reshape(rows // 8, 8, cols // 128, 128)
                sq_out[cc, to, s] = jnp.sum(jnp.sum(sq, axis=0), axis=1)
                mom_b[m] = new.astype(BF16)
            if s == 0:
                @pl.when(i > 0)
                def _():
                    send(s, i - 1)
            return carry

        lax.fori_loop(0, chips, momentum, 0)
        if s == 0:
            send_pair(s)
            load_set(1)
            for t in range(2):
                mats = pl.ds(t * group, group)
                pltpu.make_async_copy(w_hbm.at[mats], w_v.at[mats], w_sem.at[t]).start()

    swap = remote(sq_out.at[1 - core], sq_pair, qp_send.at[0], qp_recv.at[0], pair)
    swap.start()
    swap.wait()
    sq_sum[...] = sq_out[core] + sq_pair[...]
    sq_in[chip] = sq_sum[chip]
    send_pair(1)

    def send_sums(i, carry):
        to = chip_at(i)
        remote(sq_sum.at[to], sq_in.at[chip], q_send.at[0], q_recv.at[0], to * CORES + core).start()
        return carry

    def send_second(i, carry):
        @pl.when(i == 6 * core)
        def _():
            lax.fori_loop(0, chips - 1, send_sums, 0)

        send(1, i)
        return carry

    lax.fori_loop(0, chips - 1, send_second, 0)

    other_chips = pl.ds(0, chips - 1)
    half = pl.ds(0, chips)

    def owned(s, carry):
        def hand_on(i, inner):
            src = chip_at(i)
            got = x_hold.at[s, src]
            remote(got, got, a_send.at[s], a_recv.at[s, src], pair).wait_recv()
            remote(got.at[1 - core], x_v.at[s, src * CORES + core], ap_send.at[s], ap_recv.at[s], pair).start()
            return inner

        lax.fori_loop(0, chips - 1, hand_on, 0)

        @pl.when(s == 0)
        def _():
            pltpu.make_async_copy(sq_in.at[other_chips], sq_in.at[other_chips], q_recv.at[0]).wait()

        pltpu.make_async_copy(x_v.at[s, half], x_v.at[s, half], ap_recv.at[s]).wait()
        tile = sq_in[0, s]
        for j in range(1, chips):
            tile = tile + sq_in[j, s]
        total = jnp.sum(jnp.sum(tile, axis=0, keepdims=True), axis=1, keepdims=True)
        denom = jnp.sqrt(total) + NORM_EPS

        def scale(j, inner):
            same, other = j * CORES + core, j * CORES + 1 - core
            x_v[s, same] = (x_hold[s, j, core].astype(F32) / denom).astype(BF16)
            x_v[s, other] = (x_v[s, other].astype(F32) / denom).astype(BF16)
            return inner

        lax.fori_loop(0, chips, scale, 0)
        newton_schulz(x_v.at[s], gram_v, poly_v)

        def back(i, inner):
            to = chip_at(i)
            remote(x_v.at[s, pl.ds(to * CORES, CORES)], o_hold.at[s, chip], o_send.at[s], o_recv.at[s, chip], to * CORES + core).start()
            return inner

        lax.fori_loop(0, chips - 1, back, 0)
        remote(x_v.at[s, pair], o_v.at[s * group + me], op_send.at[s], op_recv.at[s], pair).start()
        o_hold[s, chip, core] = x_v[s, me]
        return carry

    lax.fori_loop(0, 2, owned, 0)

    def block(ref, s, q, src):
        return ref.at[pl.ds(s * group + q * quad_mats, quad_mats), pl.ds(pl.multiple_of(src * rows, 32), rows), :]

    def update(s):
        def hand_on(i, inner):
            src = chip_at(i)
            got = o_hold.at[s, src]
            remote(got, got, o_send.at[s], o_recv.at[s, src], pair).wait_recv()
            remote(got.at[1 - core], o_v.at[s * group + src * CORES + core], op_send.at[s], op_recv.at[s], pair).start()
            return inner

        lax.fori_loop(0, chips - 1, hand_on, 0)
        pltpu.make_async_copy(w_hbm.at[pl.ds(s * group, group)], w_v.at[pl.ds(s * group, group)], w_sem.at[s]).wait()
        pltpu.make_async_copy(o_v.at[half], o_v.at[half], op_recv.at[s]).wait()

        def one(j, carry):
            for m, ortho in (
                (s * group + j * CORES + core, o_hold[s, j, core]),
                (s * group + j * CORES + 1 - core, o_v[s * group + j * CORES + 1 - core]),
            ):
                w_old = w_v[m]
                new_v[m] = (w_old - LEARN_RATE * (ortho.astype(F32) * rms + WEIGHT_DECAY * w_old)).astype(BF16)
            return carry

        lax.fori_loop(0, chips, one, 0)
        for q in range(QUADS):
            src = new_v.at[pl.ds(s * group + q * quad_mats, quad_mats)]
            dst = block(out_hbm, s, q, me)
            remote(src, dst, ring_send.at[0], ring_recv.at[0, s, q, 0], up).start()
            remote(src, dst, ring_send.at[1], ring_recv.at[1, s, q, 0], down).start()
            remote(src, dst, pair_send.at[0], pair_recv.at[0], pair).start()
            pltpu.make_async_copy(src, dst, own_sem.at[s]).start()

    def last_hop(s, q, way):
        return RING_HOPS - 1 if s == 1 and q == HELD[way] else RING_HOPS

    def landing(s, q, way, h, src):
        if h == RING_HOPS and q % 2 == way:
            return (far_up, far_down)[way].at[pl.ds((s * (QUADS // 2) + q // 2) * quad_mats, quad_mats)]
        if h == last_hop(s, q, way) < RING_HOPS:
            return (near_up, near_down)[way]
        return block(out_hbm, s, q, src)

    def relay(s, h):
        for q in range(QUADS):
            for way in range(2):
                if h > last_hop(s, q, way):
                    continue
                src = lax.rem(chip + (chips - h if way == 0 else h), chips) * CORES + core
                got = landing(s, q, way, h, src)
                remote(got, got, ring_send.at[way], ring_recv.at[way, s, q, h - 1], (up, down)[way]).wait_recv()
                if h < last_hop(s, q, way):
                    remote(got, landing(s, q, way, h + 1, src), ring_send.at[way], ring_recv.at[way, s, q, h], (up, down)[way]).start()
                remote(got, block(out_hbm, s, q, src), pair_send.at[0], pair_recv.at[0], pair).start()

    update(0)
    relay(0, 1)
    update(1)
    relay(0, 2)
    relay(1, 1)
    relay(0, 3)
    relay(1, 2)
    relay(1, 3)

    for s in range(2):
        pltpu.make_async_copy(x_hold.at[s, other_chips], x_hold.at[s, other_chips], a_send.at[s]).wait()
        pltpu.make_async_copy(x_v.at[s, half], x_v.at[s, half], ap_send.at[s]).wait()
        pltpu.make_async_copy(o_hold.at[s, other_chips], o_hold.at[s, other_chips], o_send.at[s]).wait()
        pltpu.make_async_copy(o_v.at[half], o_v.at[half], op_send.at[s]).wait()
        own = new_v.at[pl.ds(s * group, group)]
        pltpu.make_async_copy(own, own, own_sem.at[s]).wait()
    pltpu.make_async_copy(sq_in.at[other_chips], sq_in.at[other_chips], q_send.at[0]).wait()
    for way in range(2):
        full = out_hbm.at[pl.ds(0, RING_HOPS * 2 * QUADS - 1), pl.ds(0, quad_mats * rows)]
        pltpu.make_async_copy(full, full, ring_send.at[way]).wait()
    full = out_hbm.at[pl.ds(0, (2 * RING_HOPS + 1) * QUADS - 1), pl.ds(0, 2 * quad_mats * rows)]
    pltpu.make_async_copy(full, full, pair_send.at[0]).wait()
    pltpu.make_async_copy(full, full, pair_recv.at[0]).wait()


def lay_first_kernel(group, gath, far_up, far_down, near_up, near_down, mom_hbm, grad_hbm, out_hbm, mom_out,
                     buf, in_sem, out_sem, mom_v, grad_v, mom_in, mom_done):
    momentum = mom_hbm, grad_hbm, mom_out, mom_v, grad_v, mom_in, mom_done
    lay_blocks(group, 0, LAID_FIRST, (gath, far_up, far_down, near_up, near_down), out_hbm, (buf, in_sem, out_sem), momentum)


def lay_rest_kernel(group, prev, gath, far_up, far_down, near_up, near_down, out_hbm, buf, in_sem, out_sem):
    total = (2 * RING_HOPS + 1) * CORES * 2 * QUADS
    lay_blocks(group, LAID_FIRST, total, (gath, far_up, far_down, near_up, near_down), out_hbm, (buf, in_sem, out_sem), None)


def lay_blocks(group, first, total, sources, out_hbm, scratch, momentum):
    gath, far_up, far_down, near_up, near_down = sources
    buf, in_sem, out_sem = scratch
    _, _, rows, _ = buf.shape
    count = gath.shape[0]
    chips = group // CORES
    quads = 2 * QUADS
    quad_mats = count // quads
    me = lax.axis_index("data")
    chip, core = me // CORES, me % CORES
    per_chip = CORES * quads
    every = (total - first) // quads
    if momentum is not None:
        mom_hbm, grad_hbm, mom_out, mom_v, grad_v, mom_in, mom_done = momentum

    def where(i):
        j, c, g = i // per_chip, (i // quads) % CORES, i % quads
        src = lax.rem(chip + j + chips - RING_HOPS, chips) * CORES + c
        return j, c, g, src

    def block(ref, g, src):
        return ref.at[pl.ds(g * quad_mats, quad_mats), pl.ds(pl.multiple_of(src * rows, 32), rows), :]

    def here(i):
        j, _, g, _ = where(i)
        return jnp.logical_not(((j == 0) & (g == QUADS + HELD[0])) | ((j == 2 * RING_HOPS) & (g == QUADS + HELD[1])))

    def load(i):
        j, c, g, src = where(i)
        slot = i % SLOTS
        up_far = (j == 0) & (c == core) & (g % 2 == 0)
        down_far = (j == 2 * RING_HOPS) & (c == core) & (g % 2 == 1)
        up_near = (j == 1) & (c == core) & (g == QUADS + HELD[0])
        down_near = (j == 2 * RING_HOPS - 1) & (c == core) & (g == QUADS + HELD[1])
        far = pl.ds((g // 2) * quad_mats, quad_mats)

        @pl.when(up_far)
        def _():
            pltpu.make_async_copy(far_up.at[far], buf.at[slot], in_sem.at[slot]).start()

        @pl.when(down_far)
        def _():
            pltpu.make_async_copy(far_down.at[far], buf.at[slot], in_sem.at[slot]).start()

        @pl.when(up_near)
        def _():
            pltpu.make_async_copy(near_up, buf.at[slot], in_sem.at[slot]).start()

        @pl.when(down_near)
        def _():
            pltpu.make_async_copy(near_down, buf.at[slot], in_sem.at[slot]).start()

        @pl.when(jnp.logical_not(up_far | down_far | up_near | down_near))
        def _():
            pltpu.make_async_copy(block(gath, g, src), buf.at[slot], in_sem.at[slot]).start()

    def store(i):
        _, _, g, src = where(i)
        slot = i % SLOTS
        return pltpu.make_async_copy(buf.at[slot], block(out_hbm, g, src), out_sem.at[slot])

    def step(i, carry):
        @pl.when((i >= first + SLOTS) & (i < total) & here(jnp.maximum(i - SLOTS, 0)))
        def _():
            store(i - SLOTS).wait()

        @pl.when((i < total) & here(i))
        def _():
            load(i)

        @pl.when((i >= first + LAG) & here(jnp.maximum(i - LAG, 0)))
        def _():
            late = (i - LAG) % SLOTS
            pltpu.make_async_copy(buf.at[late], buf.at[late], in_sem.at[late]).wait()
            store(i - LAG).start()

        if momentum is None:
            return carry
        t = i // every
        mats = pl.ds(t * quad_mats, quad_mats)

        @pl.when((i % every == 0) & (t < quads))
        def _():
            pltpu.make_async_copy(mom_hbm.at[mats], mom_v.at[mats], mom_in.at[0, t]).start()
            pltpu.make_async_copy(grad_hbm.at[mats], grad_v.at[mats], mom_in.at[1, t]).start()

        @pl.when((i % every == every - 1) & (t < quads))
        def _():
            pltpu.make_async_copy(mom_hbm.at[mats], mom_v.at[mats], mom_in.at[0, t]).wait()
            pltpu.make_async_copy(grad_hbm.at[mats], grad_v.at[mats], mom_in.at[1, t]).wait()

            def one(m, inner):
                mom_v[m] = MOMENTUM * mom_v[m] + grad_v[m].astype(F32)
                return inner

            lax.fori_loop(t * quad_mats, (t + 1) * quad_mats, one, 0)
            pltpu.make_async_copy(mom_v.at[mats], mom_out.at[mats], mom_done.at[t]).start()

        return carry

    lax.fori_loop(first, total + LAG, step, 0)

    def drain(i, carry):
        @pl.when(here(i))
        def _():
            store(i).wait()

        return carry

    lax.fori_loop(total - SLOTS, total, drain, 0)
    for t in range(quads if momentum is not None else 0):
        mats = pl.ds(t * quad_mats, quad_mats)
        pltpu.make_async_copy(mom_v.at[mats], mom_out.at[mats], mom_done.at[t]).wait()


def place_kernel(group, pieces, prev, own_up, own_down, pair_up, pair_down, out_hbm, out_sem):
    count = prev.shape[0]
    _, rows, _ = own_up.shape
    chips = group // CORES
    quad_mats = count // (2 * QUADS)
    me = lax.axis_index("data")
    chip, core = me // CORES, me % CORES
    late = (own_up, own_down), (pair_up, pair_down)

    def store(n, other):
        way, place_in, g, away = pieces[n]
        src = lax.rem(chip + away, chips) * CORES + (1 - core if other else core)
        rows_of = pl.ds(pl.multiple_of(src * rows, 32), rows)
        got = late[other][way].at[pl.ds(place_in * quad_mats, quad_mats)]
        return pltpu.make_async_copy(got, out_hbm.at[pl.ds(g * quad_mats, quad_mats), rows_of, :], out_sem.at[other, n])

    for other in range(2):
        for n in range(len(pieces)):
            store(n, other).start()
    for other in range(2):
        for n in range(len(pieces)):
            store(n, other).wait()


def lay_first(group, gathered, mom_rows, grad_rows):
    count, rows, cols = mom_rows.shape
    quads = 2 * QUADS
    any_spec = pl.BlockSpec(memory_space=pltpu.HBM)
    dma = pltpu.SemaphoreType.DMA
    size = gathered[0].size
    return pl.pallas_call(
        functools.partial(lay_first_kernel, group),
        out_shape=(jax.ShapeDtypeStruct(gathered[0].shape, BF16), jax.ShapeDtypeStruct((count, rows, cols), F32)),
        in_specs=[any_spec] * 7,
        out_specs=(any_spec, any_spec),
        scratch_shapes=[
            pltpu.VMEM((SLOTS, count // quads, rows, cols), BF16), dma((SLOTS,)), dma((SLOTS,)),
            pltpu.VMEM((count, rows, cols), F32), pltpu.VMEM((count, rows, cols), BF16), dma((2, quads)), dma((quads,)),
        ],
        compiler_params=pltpu.CompilerParams(vmem_limit_bytes=58 * 1024 * 1024),
        cost_estimate=pl.CostEstimate(flops=200_000_000, bytes_accessed=4 * size, transcendentals=0),
        name="lay_first",
    )(*gathered, mom_rows, grad_rows)


def lay_rest(group, prev, gathered):
    count = prev.shape[0]
    quads = 2 * QUADS
    _, rows, cols = gathered[1].shape
    any_spec = pl.BlockSpec(memory_space=pltpu.HBM)
    dma = pltpu.SemaphoreType.DMA
    return pl.pallas_call(
        functools.partial(lay_rest_kernel, group),
        out_shape=jax.ShapeDtypeStruct(prev.shape, BF16),
        in_specs=[any_spec] * 6,
        out_specs=any_spec,
        input_output_aliases={0: 0},
        scratch_shapes=[pltpu.VMEM((SLOTS, count // quads, rows, cols), BF16), dma((SLOTS,)), dma((SLOTS,))],
        compiler_params=pltpu.CompilerParams(vmem_limit_bytes=54 * 1024 * 1024),
        cost_estimate=pl.CostEstimate(flops=40_000_000, bytes_accessed=prev.size, transcendentals=0),
        name="lay_rest",
    )(prev, *gathered)


def place(group, near, prev, late):
    chips = group // CORES
    if near:
        pieces = [(0, 0, QUADS + HELD[0], chips - RING_HOPS), (1, 0, QUADS + HELD[1], RING_HOPS)]
    else:
        pieces = [(g % 2, g // 2, g, chips // 2) for g in range(2 * QUADS)]
    any_spec = pl.BlockSpec(memory_space=pltpu.HBM)
    return pl.pallas_call(
        functools.partial(place_kernel, group, pieces),
        out_shape=jax.ShapeDtypeStruct(prev.shape, BF16),
        in_specs=[any_spec] + [pl.BlockSpec(memory_space=pl.ANY)] * 4,
        out_specs=any_spec,
        input_output_aliases={0: 0},
        scratch_shapes=[pltpu.SemaphoreType.DMA((2, len(pieces)))],
        compiler_params=pltpu.CompilerParams(vmem_limit_bytes=4 * 1024 * 1024),
        cost_estimate=pl.CostEstimate(flops=20_000_000, bytes_accessed=16 * late[0].size, transcendentals=0),
        name="place_near" if near else "place_far",
    )(prev, *late)


def run_step(group, w_rows, mom_rows, grad_rows):
    count, rows, cols = mom_rows.shape
    chips = group // CORES
    any_spec = pl.BlockSpec(memory_space=pltpu.HBM)
    dma = pltpu.SemaphoreType.DMA
    return pl.pallas_call(
        functools.partial(step_kernel, group),
        out_shape=(
            jax.ShapeDtypeStruct((count, rows * group, cols), BF16),
            jax.ShapeDtypeStruct((count // 2, rows, cols), BF16),
            jax.ShapeDtypeStruct((count // 2, rows, cols), BF16),
            jax.ShapeDtypeStruct((group // QUADS, rows, cols), BF16),
            jax.ShapeDtypeStruct((group // QUADS, rows, cols), BF16),
        ),
        in_specs=[any_spec] * 3,
        out_specs=(any_spec,) * 5,
        scratch_shapes=[
            pltpu.VMEM((count, rows, cols), F32),
            pltpu.VMEM((count, rows, cols), BF16),
            pltpu.VMEM((count, rows, cols), F32),
            pltpu.VMEM((count, rows, cols), BF16),
            pltpu.VMEM((2, group, rows, cols), BF16),
            pltpu.VMEM((2, chips, CORES, rows, cols), BF16),
            pltpu.VMEM((count, rows, cols), BF16),
            pltpu.VMEM((2, chips, CORES, rows, cols), BF16),
            pltpu.VMEM((count, rows, cols), BF16),
            pltpu.VMEM((CORES, chips, 2, 8, 128), F32),
            pltpu.VMEM((chips, 2, 8, 128), F32),
            pltpu.VMEM((chips, 2, 8, 128), F32),
            pltpu.VMEM((chips, 2, 8, 128), F32),
            pltpu.VMEM((cols, cols), BF16),
            pltpu.VMEM((cols, cols), BF16),
            dma((2, count)), dma((2,)),
            dma((2,)), dma((2, chips)), dma((2,)), dma((2,)), dma((1,)), dma((1,)), dma((1,)), dma((1,)),
            dma((2,)), dma((2, chips)), dma((2,)), dma((2,)),
            dma((2,)), dma((2, 2, QUADS, RING_HOPS)), dma((1,)), dma((1,)), dma((2,)),
        ],
        compiler_params=pltpu.CompilerParams(collective_id=0, has_side_effects=True, vmem_limit_bytes=60 * 1024 * 1024),
        name="muon_step",
    )(w_rows, mom_rows, grad_rows)


def solution(mesh):
    group = mesh.shape["data"]
    row_spec = P("stage", "data", None)
    full_spec = P("stage", None, None)

    def local_step(w_rows, mom_rows, grad_rows):
        gath, far_up, far_down, near_up, near_down = run_step(group, w_rows, mom_rows, grad_rows)
        upward = [(d, (d + CORES) % group) for d in range(group)]
        downward = [(d, (d - CORES) % group) for d in range(group)]
        pairs = [(d, d ^ 1) for d in range(group)]

        def hop(arr, perm):
            return lax.ppermute(arr, "data", perm)

        far = hop(far_up, upward), hop(far_down, downward)
        near = hop(near_up, upward), hop(near_down, downward)
        gathered = gath, far_up, far_down, near_up, near_down
        params, mom_new = lay_first(group, gathered, mom_rows, grad_rows)
        far_u, far_d, params = lax.optimization_barrier(far + (params,))
        far_pair = hop(far_u, pairs), hop(far_d, pairs)
        params = lay_rest(group, params, gathered)
        near_u, near_d, params = lax.optimization_barrier(near + (params,))
        near_pair = hop(near_u, pairs), hop(near_d, pairs)
        params = place(group, False, params, (far_u, far_d) + far_pair)
        params = place(group, True, params, (near_u, near_d) + near_pair)
        return params, mom_new

    return jax.shard_map(local_step, mesh=mesh, in_specs=(row_spec, row_spec, row_spec), out_specs=(full_spec, row_spec), check_vma=False)
```

```python
import functools
import math
import jax
import jax.numpy as jnp
from jax import lax
from jax.experimental import pallas as pl
from jax.experimental.pallas import tpu as pltpu
from jax.sharding import PartitionSpec as P

NS_ITERS = 5
MOMENTUM = 0.95
LEARN_RATE = 0.02
WEIGHT_DECAY = 0.1
NORM_EPS = 1e-7
COEF_A = 3.4445
COEF_B = -4.7750
COEF_C = 2.0315
CORES = 2
QUADS = 4
MESH = pl.DeviceIdType.MESH
F32 = jnp.float32
BF16 = jnp.bfloat16


RING_HOPS = 3
HELD = (QUADS - 1, QUADS - 2)
LAY_MIB = 55
SLOTS = 24
LAG = 12


def newton_schulz(x_ref, gram_ref, poly_ref):
    blocks, rows, cols = x_ref.shape
    half = cols // 2
    step = blocks // 4

    def iteration(i, carry):
        x_all = x_ref[...].reshape(blocks * rows, cols)
        gram_ref[...] = lax.dot_general(
            x_all, x_all, (((0,), (0,)), ((), ())), preferred_element_type=F32
        ).astype(BF16)
        gram = gram_ref[...]
        for p in range(2):
            part = gram_ref[p * half:(p + 1) * half, :]
            square = jnp.dot(part, gram, preferred_element_type=F32)
            poly_ref[p * half:(p + 1) * half, :] = (COEF_B * part.astype(F32) + COEF_C * square).astype(BF16)
        poly = poly_ref[...]

        def rows_of(r, inner):
            x_part = x_ref[pl.ds(r * step, step)].reshape(step * rows, cols)
            prod = jnp.dot(x_part, poly, preferred_element_type=F32)
            x_ref[pl.ds(r * step, step)] = (COEF_A * x_part.astype(F32) + prod).astype(BF16).reshape(step, rows, cols)
            return inner

        for r in range(4):
            rows_of(r, 0)
        return carry

    lax.fori_loop(0, NS_ITERS, iteration, 0)


def step_kernel(group, w_hbm, mom_hbm, grad_hbm, out_hbm, far_up, far_down, near_up, near_down,
                mom_v, grad_v, w_v, mom_b, x_v, x_hold, o_v, o_hold, new_v, sq_out, sq_pair, sq_sum, sq_in, gram_v, poly_v,
                in_sem, w_sem, a_send, a_recv, ap_send, ap_recv, q_send, q_recv, qp_send, qp_recv,
                o_send, o_recv, op_send, op_recv, ring_send, ring_recv, pair_send, pair_recv, own_sem):
    _, rows, cols = mom_hbm.shape
    chips = group // CORES
    quad_mats = group // QUADS
    rms = 0.2 * math.sqrt(max(rows * group, cols))
    me = lax.axis_index("data")
    chip, core = me // CORES, me % CORES
    up = lax.rem(chip + 1, chips) * CORES + core
    down = lax.rem(chip + chips - 1, chips) * CORES + core
    pair = chip * CORES + (1 - core)

    def chip_at(i):
        return lax.rem(chip + chips // 2 + (i + 1) // 2 * (1 - 2 * (i % 2)), chips)

    def remote(src, dst, send_sem, recv_sem, to):
        return pltpu.make_async_remote_copy(src, dst, send_sem, recv_sem, device_id={"data": to}, device_id_type=MESH)

    barrier = pltpu.get_barrier_semaphore()

    def greet(i, carry):
        pl.semaphore_signal(barrier, inc=1, device_id={"data": chip_at(i) * CORES + core}, device_id_type=MESH)
        return carry

    lax.fori_loop(0, chips - 1, greet, 0)
    pl.semaphore_signal(barrier, inc=1, device_id={"data": pair}, device_id_type=MESH)

    def load_set(s):
        def load(i, carry):
            for cc in range(CORES):
                m = s * group + chip_at(i) * CORES + cc
                pltpu.make_async_copy(mom_hbm.at[m], mom_v.at[m], in_sem.at[0, m]).start()
                pltpu.make_async_copy(grad_hbm.at[m], grad_v.at[m], in_sem.at[1, m]).start()
            return carry

        lax.fori_loop(0, chips, load, 0)

    load_set(0)
    pl.semaphore_wait(barrier, chips)

    def send(s, i):
        to = chip_at(i)
        src = mom_b.at[pl.ds(s * group + to * CORES, CORES)]
        remote(src, x_hold.at[s, chip], a_send.at[s], a_recv.at[s, chip], to * CORES + core).start()

    def send_pair(s):
        remote(mom_b.at[s * group + pair], x_v.at[s, me], ap_send.at[s], ap_recv.at[s], pair).start()
        x_hold[s, chip, core] = mom_b[s * group + me]

    for s in range(2):
        def momentum(i, carry):
            to = chip_at(i)
            for cc in range(CORES):
                m = s * group + to * CORES + cc
                pltpu.make_async_copy(mom_hbm.at[m], mom_v.at[m], in_sem.at[0, m]).wait()
                pltpu.make_async_copy(grad_hbm.at[m], grad_v.at[m], in_sem.at[1, m]).wait()
                new = MOMENTUM * mom_v[m] + grad_v[m].astype(F32)
                sq = (new * new).reshape(rows // 8, 8, cols // 128, 128)
                sq_out[cc, to, s] = jnp.sum(jnp.sum(sq, axis=0), axis=1)
                mom_b[m] = new.astype(BF16)
            if s == 0:
                @pl.when(i > 0)
                def _():
                    send(s, i - 1)
            return carry

        lax.fori_loop(0, chips, momentum, 0)
        if s == 0:
            send_pair(s)
            load_set(1)
            for t in range(2):
                mats = pl.ds(t * group, group)
                pltpu.make_async_copy(w_hbm.at[mats], w_v.at[mats], w_sem.at[t]).start()

    swap = remote(sq_out.at[1 - core], sq_pair, qp_send.at[0], qp_recv.at[0], pair)
    swap.start()
    swap.wait()
    sq_sum[...] = sq_out[core] + sq_pair[...]
    sq_in[chip] = sq_sum[chip]
    send_pair(1)

    def send_sums(i, carry):
        to = chip_at(i)
        remote(sq_sum.at[to], sq_in.at[chip], q_send.at[0], q_recv.at[0], to * CORES + core).start()
        return carry

    def send_second(i, carry):
        @pl.when(i == 6 * core)
        def _():
            lax.fori_loop(0, chips - 1, send_sums, 0)

        send(1, i)
        return carry

    lax.fori_loop(0, chips - 1, send_second, 0)

    other_chips = pl.ds(0, chips - 1)
    half = pl.ds(0, chips)

    def owned(s, carry):
        def hand_on(i, inner):
            src = chip_at(i)
            got = x_hold.at[s, src]
            remote(got, got, a_send.at[s], a_recv.at[s, src], pair).wait_recv()
            remote(got.at[1 - core], x_v.at[s, src * CORES + core], ap_send.at[s], ap_recv.at[s], pair).start()
            return inner

        lax.fori_loop(0, chips - 1, hand_on, 0)

        @pl.when(s == 0)
        def _():
            pltpu.make_async_copy(sq_in.at[other_chips], sq_in.at[other_chips], q_recv.at[0]).wait()

        pltpu.make_async_copy(x_v.at[s, half], x_v.at[s, half], ap_recv.at[s]).wait()
        tile = sq_in[0, s]
        for j in range(1, chips):
            tile = tile + sq_in[j, s]
        total = jnp.sum(jnp.sum(tile, axis=0, keepdims=True), axis=1, keepdims=True)
        denom = jnp.sqrt(total) + NORM_EPS

        def scale(j, inner):
            same, other = j * CORES + core, j * CORES + 1 - core
            x_v[s, same] = (x_hold[s, j, core].astype(F32) / denom).astype(BF16)
            x_v[s, other] = (x_v[s, other].astype(F32) / denom).astype(BF16)
            return inner

        lax.fori_loop(0, chips, scale, 0)
        newton_schulz(x_v.at[s], gram_v, poly_v)

        def back(i, inner):
            to = chip_at(i)
            remote(x_v.at[s, pl.ds(to * CORES, CORES)], o_hold.at[s, chip], o_send.at[s], o_recv.at[s, chip], to * CORES + core).start()
            return inner

        lax.fori_loop(0, chips - 1, back, 0)
        remote(x_v.at[s, pair], o_v.at[s * group + me], op_send.at[s], op_recv.at[s], pair).start()
        o_hold[s, chip, core] = x_v[s, me]
        return carry

    lax.fori_loop(0, 2, owned, 0)

    def block(ref, s, q, src):
        return ref.at[pl.ds(s * group + q * quad_mats, quad_mats), pl.ds(pl.multiple_of(src * rows, 32), rows), :]

    def update(s):
        def hand_on(i, inner):
            src = chip_at(i)
            got = o_hold.at[s, src]
            remote(got, got, o_send.at[s], o_recv.at[s, src], pair).wait_recv()
            remote(got.at[1 - core], o_v.at[s * group + src * CORES + core], op_send.at[s], op_recv.at[s], pair).start()
            return inner

        lax.fori_loop(0, chips - 1, hand_on, 0)
        pltpu.make_async_copy(w_hbm.at[pl.ds(s * group, group)], w_v.at[pl.ds(s * group, group)], w_sem.at[s]).wait()
        pltpu.make_async_copy(o_v.at[half], o_v.at[half], op_recv.at[s]).wait()

        def one(j, carry):
            for m, ortho in (
                (s * group + j * CORES + core, o_hold[s, j, core]),
                (s * group + j * CORES + 1 - core, o_v[s * group + j * CORES + 1 - core]),
            ):
                w_old = w_v[m]
                new_v[m] = (w_old - LEARN_RATE * (ortho.astype(F32) * rms + WEIGHT_DECAY * w_old)).astype(BF16)
            return carry

        lax.fori_loop(0, chips, one, 0)
        for q in range(QUADS):
            src = new_v.at[pl.ds(s * group + q * quad_mats, quad_mats)]
            dst = block(out_hbm, s, q, me)
            remote(src, dst, ring_send.at[0], ring_recv.at[0, s, q, 0], up).start()
            remote(src, dst, ring_send.at[1], ring_recv.at[1, s, q, 0], down).start()
            remote(src, dst, pair_send.at[0], pair_recv.at[0], pair).start()
            pltpu.make_async_copy(src, dst, own_sem.at[s]).start()

    def last_hop(s, q, way):
        return RING_HOPS - 1 if s == 1 and q == HELD[way] else RING_HOPS

    def landing(s, q, way, h, src):
        if h == RING_HOPS and q % 2 == way:
            return (far_up, far_down)[way].at[pl.ds((s * (QUADS // 2) + q // 2) * quad_mats, quad_mats)]
        if h == last_hop(s, q, way) < RING_HOPS:
            return (near_up, near_down)[way]
        return block(out_hbm, s, q, src)

    def relay(s, h):
        for q in range(QUADS):
            for way in range(2):
                if h > last_hop(s, q, way):
                    continue
                src = lax.rem(chip + (chips - h if way == 0 else h), chips) * CORES + core
                got = landing(s, q, way, h, src)
                remote(got, got, ring_send.at[way], ring_recv.at[way, s, q, h - 1], (up, down)[way]).wait_recv()
                if h < last_hop(s, q, way):
                    remote(got, landing(s, q, way, h + 1, src), ring_send.at[way], ring_recv.at[way, s, q, h], (up, down)[way]).start()
                if not (h == RING_HOPS and q % 2 == way):
                    remote(got, block(out_hbm, s, q, src), pair_send.at[0], pair_recv.at[0], pair).start()

    update(0)
    relay(0, 1)
    update(1)
    relay(0, 2)
    relay(1, 1)
    relay(0, 3)
    relay(1, 2)
    relay(1, 3)

    for s in range(2):
        pltpu.make_async_copy(x_hold.at[s, other_chips], x_hold.at[s, other_chips], a_send.at[s]).wait()
        pltpu.make_async_copy(x_v.at[s, half], x_v.at[s, half], ap_send.at[s]).wait()
        pltpu.make_async_copy(o_hold.at[s, other_chips], o_hold.at[s, other_chips], o_send.at[s]).wait()
        pltpu.make_async_copy(o_v.at[half], o_v.at[half], op_send.at[s]).wait()
        own = new_v.at[pl.ds(s * group, group)]
        pltpu.make_async_copy(own, own, own_sem.at[s]).wait()
    pltpu.make_async_copy(sq_in.at[other_chips], sq_in.at[other_chips], q_send.at[0]).wait()
    for way in range(2):
        full = out_hbm.at[pl.ds(0, RING_HOPS * 2 * QUADS - 1), pl.ds(0, quad_mats * rows)]
        pltpu.make_async_copy(full, full, ring_send.at[way]).wait()
    full = out_hbm.at[pl.ds(0, 2 * RING_HOPS * QUADS - 1), pl.ds(0, 2 * quad_mats * rows)]
    pltpu.make_async_copy(full, full, pair_send.at[0]).wait()
    pltpu.make_async_copy(full, full, pair_recv.at[0]).wait()


def lay_kernel(group, gath, far_up, far_down, near_up, near_down, mom_hbm, grad_hbm, out_hbm, mom_out,
               buf, in_sem, out_sem, mom_v, grad_v, mom_in, mom_done):
    _, _, rows, _ = buf.shape
    count = gath.shape[0]
    chips = group // CORES
    quads = 2 * QUADS
    quad_mats = count // quads
    me = lax.axis_index("data")
    chip, core = me // CORES, me % CORES
    per_chip = CORES * quads
    total = (2 * RING_HOPS + 1) * per_chip
    every = total // quads

    def where(i):
        j, c, g = i // per_chip, (i // quads) % CORES, i % quads
        src = lax.rem(chip + j + chips - RING_HOPS, chips) * CORES + c
        return j, c, g, src

    def block(ref, g, src):
        return ref.at[pl.ds(g * quad_mats, quad_mats), pl.ds(pl.multiple_of(src * rows, 32), rows), :]

    def here(i):
        j, c, g, _ = where(i)
        held = ((j == 0) & (g == QUADS + HELD[0])) | ((j == 2 * RING_HOPS) & (g == QUADS + HELD[1]))
        paired = (c != core) & (((j == 0) & (g % 2 == 0)) | ((j == 2 * RING_HOPS) & (g % 2 == 1)))
        return jnp.logical_not(held | paired)

    def load(i):
        j, c, g, src = where(i)
        slot = i % SLOTS
        up_far = (j == 0) & (c == core) & (g % 2 == 0)
        down_far = (j == 2 * RING_HOPS) & (c == core) & (g % 2 == 1)
        up_near = (j == 1) & (c == core) & (g == QUADS + HELD[0])
        down_near = (j == 2 * RING_HOPS - 1) & (c == core) & (g == QUADS + HELD[1])
        far = pl.ds((g // 2) * quad_mats, quad_mats)

        @pl.when(up_far)
        def _():
            pltpu.make_async_copy(far_up.at[far], buf.at[slot], in_sem.at[slot]).start()

        @pl.when(down_far)
        def _():
            pltpu.make_async_copy(far_down.at[far], buf.at[slot], in_sem.at[slot]).start()

        @pl.when(up_near)
        def _():
            pltpu.make_async_copy(near_up, buf.at[slot], in_sem.at[slot]).start()

        @pl.when(down_near)
        def _():
            pltpu.make_async_copy(near_down, buf.at[slot], in_sem.at[slot]).start()

        @pl.when(jnp.logical_not(up_far | down_far | up_near | down_near))
        def _():
            pltpu.make_async_copy(block(gath, g, src), buf.at[slot], in_sem.at[slot]).start()

    def store(i):
        _, _, g, src = where(i)
        slot = i % SLOTS
        return pltpu.make_async_copy(buf.at[slot], block(out_hbm, g, src), out_sem.at[slot])

    def step(i, carry):
        @pl.when((i >= SLOTS) & (i < total) & here(jnp.maximum(i - SLOTS, 0)))
        def _():
            store(i - SLOTS).wait()

        @pl.when((i < total) & here(i))
        def _():
            load(i)

        @pl.when((i >= LAG) & here(jnp.maximum(i - LAG, 0)))
        def _():
            late = (i - LAG) % SLOTS
            pltpu.make_async_copy(buf.at[late], buf.at[late], in_sem.at[late]).wait()
            store(i - LAG).start()

        t = i // every
        mats = pl.ds(t * quad_mats, quad_mats)

        @pl.when((i % every == 0) & (t < quads))
        def _():
            pltpu.make_async_copy(mom_hbm.at[mats], mom_v.at[mats], mom_in.at[0, t]).start()
            pltpu.make_async_copy(grad_hbm.at[mats], grad_v.at[mats], mom_in.at[1, t]).start()

        @pl.when((i % every == every - 1) & (t < quads))
        def _():
            pltpu.make_async_copy(mom_hbm.at[mats], mom_v.at[mats], mom_in.at[0, t]).wait()
            pltpu.make_async_copy(grad_hbm.at[mats], grad_v.at[mats], mom_in.at[1, t]).wait()

            def one(m, inner):
                mom_v[m] = MOMENTUM * mom_v[m] + grad_v[m].astype(F32)
                return inner

            lax.fori_loop(t * quad_mats, (t + 1) * quad_mats, one, 0)
            pltpu.make_async_copy(mom_v.at[mats], mom_out.at[mats], mom_done.at[t]).start()

        return carry

    lax.fori_loop(0, total + LAG, step, 0)

    def drain(i, carry):
        @pl.when(here(i))
        def _():
            store(i).wait()

        return carry

    lax.fori_loop(total - SLOTS, total, drain, 0)
    for t in range(quads):
        mats = pl.ds(t * quad_mats, quad_mats)
        pltpu.make_async_copy(mom_v.at[mats], mom_out.at[mats], mom_done.at[t]).wait()


def place_kernel(group, other, pieces, prev, ups, downs, out_hbm, sems):
    count = prev.shape[0]
    _, rows, _ = ups.shape
    chips = group // CORES
    quad_mats = count // (2 * QUADS)
    me = lax.axis_index("data")
    chip, core = me // CORES, me % CORES

    def store(n):
        way, place_in, g, away = pieces[n]
        src = lax.rem(chip + away, chips) * CORES + (1 - core if other else core)
        rows_of = pl.ds(pl.multiple_of(src * rows, 32), rows)
        got = (ups, downs)[way].at[pl.ds(place_in * quad_mats, quad_mats)]
        return pltpu.make_async_copy(got, out_hbm.at[pl.ds(g * quad_mats, quad_mats), rows_of, :], sems.at[n])

    for n in range(len(pieces)):
        store(n).start()
    for n in range(len(pieces)):
        store(n).wait()


def lay(group, gathered, mom_rows, grad_rows):
    count, rows, cols = mom_rows.shape
    quads = 2 * QUADS
    any_spec = pl.BlockSpec(memory_space=pltpu.HBM)
    dma = pltpu.SemaphoreType.DMA
    size = gathered[0].size
    return pl.pallas_call(
        functools.partial(lay_kernel, group),
        out_shape=(jax.ShapeDtypeStruct(gathered[0].shape, BF16), jax.ShapeDtypeStruct((count, rows, cols), F32)),
        in_specs=[any_spec] * 7,
        out_specs=(any_spec, any_spec),
        scratch_shapes=[
            pltpu.VMEM((SLOTS, count // quads, rows, cols), BF16), dma((SLOTS,)), dma((SLOTS,)),
            pltpu.VMEM((count, rows, cols), F32), pltpu.VMEM((count, rows, cols), BF16), dma((2, quads)), dma((quads,)),
        ],
        compiler_params=pltpu.CompilerParams(vmem_limit_bytes=LAY_MIB * 1024 * 1024),
        cost_estimate=pl.CostEstimate(flops=200_000_000, bytes_accessed=4 * size, transcendentals=0),
        name="lay",
    )(*gathered, mom_rows, grad_rows)


def place(group, kind, other, prev, ups, downs):
    chips = group // CORES
    if kind == "last":
        pieces = [(g % 2, g // 2, g, chips - RING_HOPS if g % 2 == 0 else RING_HOPS) for g in range(2 * QUADS)]
    elif kind == "near":
        pieces = [(0, 0, QUADS + HELD[0], chips - RING_HOPS), (1, 0, QUADS + HELD[1], RING_HOPS)]
    else:
        pieces = [(g % 2, g // 2, g, chips // 2) for g in range(2 * QUADS)]
    any_spec = pl.BlockSpec(memory_space=pltpu.HBM)
    return pl.pallas_call(
        functools.partial(place_kernel, group, other, pieces),
        out_shape=jax.ShapeDtypeStruct(prev.shape, BF16),
        in_specs=[any_spec] + [pl.BlockSpec(memory_space=pl.ANY)] * 2,
        out_specs=any_spec,
        input_output_aliases={0: 0},
        scratch_shapes=[pltpu.SemaphoreType.DMA((len(pieces),))],
        compiler_params=pltpu.CompilerParams(vmem_limit_bytes=4 * 1024 * 1024),
        cost_estimate=pl.CostEstimate(flops=20_000_000, bytes_accessed=8 * ups.size, transcendentals=0),
    )(prev, ups, downs)


def run_step(group, w_rows, mom_rows, grad_rows):
    count, rows, cols = mom_rows.shape
    chips = group // CORES
    any_spec = pl.BlockSpec(memory_space=pltpu.HBM)
    dma = pltpu.SemaphoreType.DMA
    return pl.pallas_call(
        functools.partial(step_kernel, group),
        out_shape=(
            jax.ShapeDtypeStruct((count, rows * group, cols), BF16),
            jax.ShapeDtypeStruct((count // 2, rows, cols), BF16),
            jax.ShapeDtypeStruct((count // 2, rows, cols), BF16),
            jax.ShapeDtypeStruct((group // QUADS, rows, cols), BF16),
            jax.ShapeDtypeStruct((group // QUADS, rows, cols), BF16),
        ),
        in_specs=[any_spec] * 3,
        out_specs=(any_spec,) * 5,
        scratch_shapes=[
            pltpu.VMEM((count, rows, cols), F32),
            pltpu.VMEM((count, rows, cols), BF16),
            pltpu.VMEM((count, rows, cols), F32),
            pltpu.VMEM((count, rows, cols), BF16),
            pltpu.VMEM((2, group, rows, cols), BF16),
            pltpu.VMEM((2, chips, CORES, rows, cols), BF16),
            pltpu.VMEM((count, rows, cols), BF16),
            pltpu.VMEM((2, chips, CORES, rows, cols), BF16),
            pltpu.VMEM((count, rows, cols), BF16),
            pltpu.VMEM((CORES, chips, 2, 8, 128), F32),
            pltpu.VMEM((chips, 2, 8, 128), F32),
            pltpu.VMEM((chips, 2, 8, 128), F32),
            pltpu.VMEM((chips, 2, 8, 128), F32),
            pltpu.VMEM((cols, cols), BF16),
            pltpu.VMEM((cols, cols), BF16),
            dma((2, count)), dma((2,)),
            dma((2,)), dma((2, chips)), dma((2,)), dma((2,)), dma((1,)), dma((1,)), dma((1,)), dma((1,)),
            dma((2,)), dma((2, chips)), dma((2,)), dma((2,)),
            dma((2,)), dma((2, 2, QUADS, RING_HOPS)), dma((1,)), dma((1,)), dma((2,)),
        ],
        compiler_params=pltpu.CompilerParams(collective_id=0, has_side_effects=True, vmem_limit_bytes=60 * 1024 * 1024),
        name="muon_step",
    )(w_rows, mom_rows, grad_rows)


def solution(mesh):
    group = mesh.shape["data"]
    row_spec = P("stage", "data", None)
    full_spec = P("stage", None, None)

    def local_step(w_rows, mom_rows, grad_rows):
        gath, far_up, far_down, near_up, near_down = run_step(group, w_rows, mom_rows, grad_rows)
        upward = [(d, (d + CORES) % group) for d in range(group)]
        downward = [(d, (d - CORES) % group) for d in range(group)]
        pairs = [(d, d ^ 1) for d in range(group)]

        def hop(arr, perm):
            return lax.ppermute(arr, "data", perm)

        far = hop(far_up, upward), hop(far_down, downward)
        near = hop(near_up, upward), hop(near_down, downward)
        last_u, last_d = hop(far_up, pairs), hop(far_down, pairs)
        gathered = gath, far_up, far_down, near_up, near_down
        params, mom_new = lay(group, gathered, mom_rows, grad_rows)
        far_u, far_d, params = lax.optimization_barrier(far + (params,))
        pair_u, pair_d = hop(far_u, pairs), hop(far_d, pairs)
        params = place(group, "last", True, params, last_u, last_d)
        params = place(group, "far", False, params, far_u, far_d)
        params = place(group, "far", True, params, pair_u, pair_d)
        near_u, near_d, params = lax.optimization_barrier(near + (params,))
        pair_u, pair_d = hop(near_u, pairs), hop(near_d, pairs)
        params = place(group, "near", False, params, near_u, near_d)
        params = place(group, "near", True, params, pair_u, pair_d)
        return params, mom_new

    return jax.shard_map(local_step, mesh=mesh, in_specs=(row_spec, row_spec, row_spec), out_specs=(full_spec, row_spec), check_vma=False)
```
